16 devices in a mesh: dp: 2 (over y, z), tp: 8 (over x, core).
Axes of the slice: x: 4, y: 2, z: 1, core: 2. Of those that a mesh axis runs over, the one named last changes fastest.
The devices are a block of a 4x4x8 slice.
Arguments:
- hidden: bfloat16 [6, 1024, 8192], P('dp', 'tp'), parts along dimension 0
- attn_gain: float32 [8192], replicated
- attn_bias: float32 [8192], replicated
- mlp_gain: float32 [8192], replicated
- mlp_bias: float32 [8192], replicated
- w_qkv: bfloat16 [8192, 8, 1152], P(None, 'tp')
- w_out: bfloat16 [8192, 8192], P('tp')
- w_up: bfloat16 [8192, 32768], P(None, 'tp')
- w_down: bfloat16 [32768, 8192], P('tp')
- positions: int32 [1024], replicated
Outputs:
- output: bfloat16 [6, 1024, 8192], P('dp', 'tp'), parts along dimension 0
There are 2 independent parts. The reference program is written for one: setup_inputs(seed, part) draws one part's arguments, and reference() takes and returns one part's arrays. A program takes and returns all parts, laid end to end along the dimension named above; an argument that names none is the same for every part.
All inputs are finite; a program needn't handle non-finite values.
Results may differ from the reference program's by a relative error of at most 0.00657861.
Values are sent between devices in bfloat16 or wider.
A program may use at most 768 MiB of HBM per device.

```python
import jax
import jax.numpy as jnp
from jax import lax

D = 8192
HEADS = 128
KV_HEADS = 8
HEAD = 64
FF = 32768
BATCH = 3
SEQ_LEN = 1024
QUERY_BLOCK = 64
HALF_HEAD = 32

GROUP_SIZE = HEADS // KV_HEADS
QKV_COLS = (GROUP_SIZE + 2) * HEAD


def setup_inputs(seed: int = 0, part: int = 0) -> dict:
    root_key = jax.random.key(seed)
    sub_keys = jax.random.split(root_key, 10)
    part_key = jax.random.fold_in(sub_keys[0], part)
    hidden = jax.random.normal(part_key, (BATCH, SEQ_LEN, D), jnp.float32).astype(jnp.bfloat16)
    attn_gain = 1.0 + 0.4 * jax.random.normal(sub_keys[1], (D,), jnp.float32)
    attn_bias = 0.4 * jax.random.normal(sub_keys[2], (D,), jnp.float32)
    mlp_gain = 1.0 + 0.4 * jax.random.normal(sub_keys[3], (D,), jnp.float32)
    mlp_bias = 0.4 * jax.random.normal(sub_keys[4], (D,), jnp.float32)
    w_qkv = (1.2 * D ** -0.5 * jax.random.normal(sub_keys[5], (D, KV_HEADS, QKV_COLS), jnp.float32)).astype(jnp.bfloat16)
    w_out = (2.0 * (HEADS * HEAD) ** -0.5 * jax.random.normal(sub_keys[6], (HEADS * HEAD, D), jnp.float32)).astype(jnp.bfloat16)
    w_up = (D ** -0.5 * jax.random.normal(sub_keys[7], (D, FF), jnp.float32)).astype(jnp.bfloat16)
    w_down = (FF ** -0.5 * jax.random.normal(sub_keys[8], (FF, D), jnp.float32)).astype(jnp.bfloat16)
    pos_gaps = jax.random.randint(sub_keys[9], (SEQ_LEN,), 1, 4, jnp.int32)
    positions = (jnp.cumsum(pos_gaps) - pos_gaps[0]).astype(jnp.int32)
    return {'hidden': hidden, 'attn_gain': attn_gain, 'attn_bias': attn_bias, 'mlp_gain': mlp_gain, 'mlp_bias': mlp_bias, 'w_qkv': w_qkv, 'w_out': w_out, 'w_up': w_up, 'w_down': w_down, 'positions': positions}


def layer_norm(tok_rows, norm_gain, norm_bias):
    rows32 = tok_rows.astype(jnp.float32)
    row_mean = jnp.mean(rows32, axis=-1, keepdims=True)
    centered = rows32 - row_mean
    row_var = jnp.mean(centered * centered, axis=-1, keepdims=True)
    return (centered * lax.rsqrt(row_var + 1e-5) * norm_gain + norm_bias).astype(jnp.bfloat16)


def apply_rotary(head_vals, cos_tab, sin_tab):
    vals32 = head_vals.astype(jnp.float32)
    rotated = jnp.concatenate([-vals32[..., HALF_HEAD:], vals32[..., :HALF_HEAD]], axis=-1)
    return (vals32 * cos_tab + rotated * sin_tab).astype(jnp.bfloat16)


def attend_sequence(query_rot, key_rot, value_seq):
    key32 = key_rot.astype(jnp.float32)
    value32 = value_seq.astype(jnp.float32)
    key_idx = jnp.arange(SEQ_LEN)

    def one_block(block_idx):
        row_start = block_idx * QUERY_BLOCK
        query_blk = lax.dynamic_slice_in_dim(query_rot, row_start, QUERY_BLOCK, axis=0).astype(jnp.float32)
        scores = jnp.einsum('qkgh,skh->kgqs', query_blk, key32) * HEAD ** -0.5
        query_idx = row_start + jnp.arange(QUERY_BLOCK)
        allowed = key_idx[None, :] <= query_idx[:, None]
        scores = jnp.where(allowed, scores, -1e30)
        exp_scores = jnp.exp(scores - jnp.max(scores, axis=-1, keepdims=True))
        attn_probs = (exp_scores / jnp.sum(exp_scores, axis=-1, keepdims=True)).astype(jnp.bfloat16)
        context = jnp.einsum('kgqs,skh->qkgh', attn_probs.astype(jnp.float32), value32)
        return context.astype(jnp.bfloat16)

    ctx_blocks = lax.map(one_block, jnp.arange(SEQ_LEN // QUERY_BLOCK))
    return ctx_blocks.reshape(SEQ_LEN, HEADS * HEAD)


def reference(hidden, attn_gain, attn_bias, mlp_gain, mlp_bias, w_qkv, w_out, w_up, w_down, positions):
    inv_freq = 10000.0 ** (-2.0 * jnp.arange(HALF_HEAD, dtype=jnp.float32) / HEAD)
    angles = positions.astype(jnp.float32)[:, None] * inv_freq[None, :]
    angles = jnp.concatenate([angles, angles], axis=-1)
    cos_tab = jnp.cos(angles)
    sin_tab = jnp.sin(angles)
    w_qkv_flat = w_qkv.reshape(D, KV_HEADS * QKV_COLS)

    def one_sequence(seq_rows):
        normed_attn = layer_norm(seq_rows, attn_gain, attn_bias)
        normed_mlp = layer_norm(seq_rows, mlp_gain, mlp_bias)
        qkv_rows = jnp.dot(normed_attn, w_qkv_flat, preferred_element_type=jnp.float32).astype(jnp.bfloat16)
        qkv_rows = qkv_rows.reshape(SEQ_LEN, KV_HEADS, GROUP_SIZE + 2, HEAD)
        query_rot = apply_rotary(qkv_rows[:, :, :GROUP_SIZE, :], cos_tab[:, None, None, :], sin_tab[:, None, None, :])
        key_rot = apply_rotary(qkv_rows[:, :, GROUP_SIZE, :], cos_tab[:, None, :], sin_tab[:, None, :])
        value_seq = qkv_rows[:, :, GROUP_SIZE + 1, :]
        context = attend_sequence(query_rot, key_rot, value_seq)
        attn_part = jnp.dot(context, w_out, preferred_element_type=jnp.float32)
        up_pre = jnp.dot(normed_mlp, w_up, preferred_element_type=jnp.float32)
        up_act = jax.nn.gelu(up_pre, approximate=False).astype(jnp.bfloat16)
        mlp_part = jnp.dot(up_act, w_down, preferred_element_type=jnp.float32)
        return (seq_rows.astype(jnp.float32) + attn_part + mlp_part).astype(jnp.bfloat16)

    return lax.map(one_sequence, hidden)
```

```python
import functools

import jax
import jax.numpy as jnp
from jax import lax
from jax.experimental import pallas as pl
from jax.experimental.pallas import tpu as pltpu
from jax.sharding import PartitionSpec as P

F32 = jnp.float32
BF16 = jnp.bfloat16
LANES = 128
ROWS = 64
NORM_GROUP = 16
VMEM_LIMIT = 67_000_000


def rotary_tables(positions, head_dim):
    inv_freq = 10000.0 ** (-2.0 * jnp.arange(head_dim // 2, dtype=F32) / head_dim)
    angles = positions.astype(F32)[:, None] * inv_freq[None, :]
    cos, sin = jnp.cos(angles), jnp.sin(angles)
    cos = jnp.concatenate([cos, cos], axis=-1)
    sin = jnp.concatenate([-sin, sin], axis=-1)
    q_tab = (jnp.concatenate([cos, cos], axis=-1), jnp.concatenate([sin, sin], axis=-1))
    kv_tab = (jnp.concatenate([cos, jnp.ones_like(cos)], axis=-1), jnp.concatenate([sin, jnp.zeros_like(sin)], axis=-1))
    return q_tab + kv_tab


def rotate(vals, cos, sin, first_half):
    half = LANES // 4
    vals = vals.astype(BF16).astype(F32)
    swapped = jnp.where(first_half, pltpu.roll(vals, LANES - half, 1), pltpu.roll(vals, half, 1))
    return (vals * cos + swapped * sin).astype(BF16)


def norm_rows(x_buf, a_buf, m_buf, gains, width, rows):
    group = NORM_GROUP
    chunks = width // LANES
    a_gain, a_bias, m_gain, m_bias = gains

    def one_group(g, carry):
        at = pl.ds(pl.multiple_of(g * group, group), group)
        parts = [jnp.zeros((group, LANES), F32) for _ in range(4)]
        for c in range(chunks):
            parts[c % 4] += x_buf[at, pl.ds(c * LANES, LANES)].astype(F32)
        mean = jnp.sum(parts[0] + parts[1] + (parts[2] + parts[3]), axis=-1, keepdims=True) * (1.0 / width)
        mean = jnp.broadcast_to(mean, (group, LANES))
        parts = [jnp.zeros((group, LANES), F32) for _ in range(4)]
        for c in range(chunks):
            d = x_buf[at, pl.ds(c * LANES, LANES)].astype(F32) - mean
            parts[c % 4] += d * d
        var = jnp.sum(parts[0] + parts[1] + (parts[2] + parts[3]), axis=-1, keepdims=True) * (1.0 / width)
        rstd = jnp.broadcast_to(lax.rsqrt(var + 1e-5), (group, LANES))
        for c in range(chunks):
            cols = pl.ds(c * LANES, LANES)
            n = (x_buf[at, cols].astype(F32) - mean) * rstd
            a_buf[at, cols] = (n * a_gain[:, cols] + a_bias[:, cols]).astype(BF16)
            m_buf[at, cols] = (n * m_gain[:, cols] + m_bias[:, cols]).astype(BF16)
        return carry

    lax.fori_loop(0, rows // group, one_group, 0)


def expand_kernel(devs, width, q_tiles, up_tiles, aliased, x_hbm, a_gain, a_bias, m_gain, m_bias, wq, wkv, wu, qc, qs, kc, ks, *refs):
    refs = refs[3:] if aliased else refs
    q_out, kv_out, act_out, x_buf, a_buf, m_buf, pend, sem = refs
    m, n = pl.program_id(0), pl.program_id(1)
    rows = devs * ROWS

    def fetch(tile, start):
        for d in range(devs):
            cp = pltpu.make_async_copy(
                x_hbm.at[d, pl.ds(tile * ROWS, ROWS)], x_buf.at[pl.ds(d * ROWS, ROWS)], sem)
            cp.start() if start else cp.wait()

    @pl.when((m == 0) & (n == 0))
    def _():
        fetch(0, True)

    @pl.when(n == 0)
    def _():
        fetch(m, False)
        norm_rows(x_buf, a_buf, m_buf, (a_gain, a_bias, m_gain, m_bias), width, rows)

    @pl.when((n == 1) & (m + 1 < pl.num_programs(0)))
    def _():
        fetch(m + 1, True)

    first_half = lax.rem(lax.broadcasted_iota(jnp.int32, (rows, LANES), 1), LANES // 2) < LANES // 4

    @pl.when(n < q_tiles)
    def _():
        acc = jnp.dot(a_buf[...], wq[...], preferred_element_type=F32)
        cos, sin = qc[...].reshape(rows, LANES), qs[...].reshape(rows, LANES)
        for c in range(acc.shape[1] // LANES):
            part = rotate(acc[:, c * LANES:(c + 1) * LANES], cos, sin, first_half)
            q_out[:, :, pl.ds(c * LANES, LANES)] = part.reshape(devs, ROWS, LANES)

    @pl.when(n == q_tiles)
    def _():
        acc = jnp.dot(a_buf[...], wkv[...], preferred_element_type=F32)
        cos, sin = kc[...].reshape(rows, LANES), ks[...].reshape(rows, LANES)
        kv_out[...] = rotate(acc, cos, sin, first_half).reshape(devs, ROWS, LANES)

    def gelu_out():
        u = pend[...]
        act = 0.5 * u * (1.0 + lax.erf(u * 0.7071067811865476))
        act_out[...] = act.astype(BF16).reshape(devs, ROWS, act.shape[1])

    def up_dot():
        pend[...] = jnp.dot(m_buf[...], wu[...], preferred_element_type=F32)

    @pl.when(n == q_tiles + 1)
    def _():
        up_dot()

    @pl.when((n > q_tiles + 1) & (n <= q_tiles + up_tiles))
    def _():
        gelu_out()
        up_dot()

    @pl.when(n == q_tiles + up_tiles + 1)
    def _():
        gelu_out()


def expand(xg, row0, seq_rows, norms, w_qkv, w_up, tabs, prev):
    devs, chunk, width = xg.shape
    q_cols = w_qkv.shape[1] - LANES
    up_cols = w_up.shape[1]
    tq, tu = min(256, q_cols), min(512, up_cols)
    q_tiles, up_tiles = q_cols // tq, up_cols // tu
    m_tiles = chunk // ROWS
    h0 = row0 // ROWS
    rows = devs * ROWS
    vec = pl.BlockSpec((1, width), lambda m, n: (0, 0))
    tab = pl.BlockSpec((devs, ROWS, LANES), lambda m, n: (0, h0 + m, 0))
    any_spec = pl.BlockSpec(memory_space=pl.ANY)
    in_specs = [
        any_spec, vec, vec, vec, vec,
        pl.BlockSpec((width, tq), lambda m, n: (0, jnp.minimum(n, q_tiles - 1))),
        pl.BlockSpec((width, LANES), lambda m, n: (0, q_cols // LANES)),
        pl.BlockSpec((width, tu), lambda m, n: (0, jnp.clip(n - q_tiles - 1, 0, up_tiles - 1))),
        tab, tab, tab, tab,
    ]
    args = [xg, *norms, w_qkv, w_qkv, w_up, *tabs]
    aliases = {}
    if prev is not None:
        aliases = {len(args) + k: k for k in range(3)}
        in_specs += [any_spec] * 3
        args += list(prev)
    out_shape = [jax.ShapeDtypeStruct((devs, seq_rows, c), BF16) for c in (q_cols, LANES, up_cols)]
    out_specs = [
        pl.BlockSpec((devs, ROWS, tq), lambda m, n: (0, h0 + m, jnp.minimum(n, q_tiles - 1))),
        pl.BlockSpec((devs, ROWS, LANES), lambda m, n: (0, h0 + m, 0)),
        pl.BlockSpec((devs, ROWS, tu), lambda m, n: (0, h0 + m, jnp.clip(n - q_tiles - 2, 0, up_tiles - 1))),
    ]
    flops = 2 * devs * chunk * width * (q_cols + LANES + up_cols)
    return pl.pallas_call(
        functools.partial(expand_kernel, devs, width, q_tiles, up_tiles, prev is not None),
        grid=(m_tiles, q_tiles + up_tiles + 2),
        in_specs=in_specs,
        out_specs=out_specs,
        out_shape=out_shape,
        scratch_shapes=[
            pltpu.VMEM((rows, width), BF16), pltpu.VMEM((rows, width), BF16), pltpu.VMEM((rows, width), BF16),
            pltpu.VMEM((rows, tu), F32), pltpu.SemaphoreType.DMA,
        ],
        input_output_aliases=aliases,
        compiler_params=pltpu.CompilerParams(vmem_limit_bytes=VMEM_LIMIT),
        cost_estimate=pl.CostEstimate(flops=flops, bytes_accessed=2 * width * (q_cols + up_cols), transcendentals=0),
        name="expand",
    )(*args)


def attend_kernel(seq, head_dim, q_ref, kv_ref, out_ref, k_lo, k_hi, v_lo, v_hi):
    scale = head_dim ** -0.5

    @pl.when(pl.program_id(0) == 0)
    def _():
        kv = kv_ref[...].astype(F32)
        low = lax.broadcasted_iota(jnp.int32, kv.shape, 1) < head_dim
        keys = jnp.where(low, kv, 0.0)
        vals = jnp.where(low, 0.0, kv)
        k_lo[...] = keys.astype(BF16)
        k_hi[...] = pltpu.roll(keys, head_dim, 1).astype(BF16)
        v_hi[...] = vals.astype(BF16)
        v_lo[...] = pltpu.roll(vals, head_dim, 1).astype(BF16)

    blk = min(256, seq)
    row = lax.broadcasted_iota(jnp.int32, (blk, blk), 0)
    col = lax.broadcasted_iota(jnp.int32, (blk, blk), 1)
    allowed = col <= row
    for b in range(seq // blk):
        q = q_ref[pl.ds(b * blk, blk), :]
        keys = (b + 1) * blk
        ctx = None
        for k_ref, v_ref in ((k_lo, v_lo), (k_hi, v_hi)):
            s = lax.dot_general(q, k_ref[pl.ds(0, keys), :], (((1,), (1,)), ((), ())), preferred_element_type=F32)
            diag = jnp.where(allowed, s[:, b * blk:], -1e30)
            s = diag if b == 0 else jnp.concatenate([s[:, :b * blk], diag], axis=1)
            e = jnp.exp((s - jnp.max(s, axis=-1, keepdims=True)) * scale)
            p = (e * (1.0 / jnp.sum(e, axis=-1, keepdims=True))).astype(BF16)
            part = jnp.dot(p, v_ref[pl.ds(0, keys), :], preferred_element_type=F32)
            ctx = part if ctx is None else ctx + part
        out_ref[pl.ds(b * blk, blk), :] = ctx.astype(BF16)


def attend(q, kv, head_dim):
    seq, q_cols = q.shape
    flops = 2 * seq * seq * q_cols * 4
    return pl.pallas_call(
        functools.partial(attend_kernel, seq, head_dim),
        grid=(q_cols // LANES,),
        in_specs=[pl.BlockSpec((seq, LANES), lambda h: (0, h)), pl.BlockSpec((seq, LANES), lambda h: (0, 0))],
        out_specs=pl.BlockSpec((seq, LANES), lambda h: (0, h)),
        out_shape=jax.ShapeDtypeStruct((seq, q_cols), BF16),
        scratch_shapes=[pltpu.VMEM((seq, LANES), BF16)] * 4,
        compiler_params=pltpu.CompilerParams(vmem_limit_bytes=VMEM_LIMIT),
        cost_estimate=pl.CostEstimate(flops=flops, bytes_accessed=4 * seq * q_cols, transcendentals=0),
        name="attend",
    )(q, kv)


def contract_kernel(num, final, steps, order, ctx_hbm, act_hbm, wo, wd, *refs):
    if final:
        add, far_lo, far_hi, up_lo, up_hi, down_lo, down_hi, own, ctx_buf, act_buf, sem = refs
    else:
        send_out, ctx_buf, act_buf, sem = refs
    blk = ctx_hbm.shape[1]
    j = pl.program_id(0)

    @pl.when(j == 0)
    def _():
        cps = []
        for k in range(num):
            rows = pl.ds(k * blk, blk)
            cps.append(pltpu.make_async_copy(ctx_hbm.at[order[k]], ctx_buf.at[rows], sem))
            cps.append(pltpu.make_async_copy(act_hbm.at[order[k]], act_buf.at[rows], sem))
        for cp in cps:
            cp.start()
        for cp in cps:
            cp.wait()

    acc = jnp.dot(act_buf[...], wd[...], preferred_element_type=F32)
    acc = acc + jnp.dot(ctx_buf[...], wo[...], preferred_element_type=F32)
    acc = acc.reshape(num, blk, acc.shape[1])
    if not final:
        send_out[...] = acc.astype(BF16)
        return
    acc = acc + add[...].astype(F32)
    own[...] = acc[3]

    @pl.when(j < steps // 2)
    def _():
        far_lo[...] = acc[0].astype(BF16)
        up_lo[...] = acc[1]
        down_lo[...] = acc[2].astype(BF16)

    @pl.when(j >= steps // 2)
    def _():
        far_hi[...] = acc[0].astype(BF16)
        up_hi[...] = acc[1].astype(BF16)
        down_hi[...] = acc[2]


def contract(order, ctx, act, w_out, w_down, col0, cols, add):
    num = order.shape[0]
    devs, blk, _ = ctx.shape
    tn = min(512, cols // 2)
    steps = cols // tn
    j0 = col0 // tn
    any_spec = pl.BlockSpec(memory_space=pl.ANY)
    in_specs = [
        any_spec, any_spec,
        pl.BlockSpec((w_out.shape[0], tn), lambda j, o: (0, j0 + j)),
        pl.BlockSpec((w_down.shape[0], tn), lambda j, o: (0, j0 + j)),
    ]
    args = [order, ctx, act, w_out, w_down]
    final = add is not None
    if final:
        in_specs.append(pl.BlockSpec((num, blk, tn), lambda j, o: (0, 0, j)))
        args.append(add)
        lo = pl.BlockSpec((blk, tn), lambda j, o: (0, jnp.minimum(j, steps // 2 - 1)))
        hi = pl.BlockSpec((blk, tn), lambda j, o: (0, jnp.maximum(j - steps // 2, 0)))
        half = lambda t: jax.ShapeDtypeStruct((blk, cols // 2), t)
        out_shape = [half(BF16), half(BF16), half(F32), half(BF16), half(BF16), half(F32), jax.ShapeDtypeStruct((blk, cols), F32)]
        out_specs = [lo, hi, lo, hi, lo, hi, pl.BlockSpec((blk, tn), lambda j, o: (0, j))]
    else:
        out_shape = jax.ShapeDtypeStruct((num, blk, cols), BF16)
        out_specs = pl.BlockSpec((num, blk, tn), lambda j, o: (0, 0, j))
    depth = w_out.shape[0] + w_down.shape[0]
    return pl.pallas_call(
        functools.partial(contract_kernel, num, final, steps),
        grid_spec=pltpu.PrefetchScalarGridSpec(
            num_scalar_prefetch=1,
            grid=(steps,),
            in_specs=in_specs,
            out_specs=out_specs,
            scratch_shapes=[
                pltpu.VMEM((num * blk, w_out.shape[0]), BF16), pltpu.VMEM((num * blk, w_down.shape[0]), BF16),
                pltpu.SemaphoreType.DMA,
            ],
        ),
        out_shape=out_shape,
        compiler_params=pltpu.CompilerParams(vmem_limit_bytes=VMEM_LIMIT),
        cost_estimate=pl.CostEstimate(flops=2 * num * blk * cols * depth, bytes_accessed=2 * depth * cols, transcendentals=0),
        name="contract_own" if final else "contract_pair",
    )(*args)


def schedule(batch, spans):
    steps = []
    steps.append(("attend", 0))
    for i in range(batch - 1):
        steps += [("pair", i), ("attend", i + 1)]
        if i:
            steps.append(("merge", i - 1))
        steps.append(("own", i))
    first = batch - 1
    steps += [("pair", first)]
    for i in range(first, spans):
        if i + 1 < spans:
            steps.append(("pair", i + 1))
        steps.append(("merge", i - 1))
        steps.append(("own", i))
        if i >= 2:
            steps.append(("finish", i - 2))
    return steps + [("finish", spans - 2), ("merge", spans - 1), ("finish", spans - 1)]


def solution(mesh):
    tp = mesh.shape["tp"]
    chips = tp // 2
    assert tp == 2 * chips and chips == 4
    pair = [(i, i ^ 1) for i in range(tp)]
    up_ring = [(i, (i + 2) % tp) for i in range(tp)]
    down_ring = [(i, (i - 2) % tp) for i in range(tp)]

    def local_layer(hidden_blk, attn_gain, attn_bias, mlp_gain, mlp_bias, w_qkv_part, w_out_part, w_up_part, w_down_part, positions):
        batch, seq_rows, width = hidden_blk.shape
        seq = seq_rows * tp
        w_qkv = w_qkv_part.reshape(width, w_qkv_part.shape[2])
        q_cols = w_out_part.shape[0]
        head_dim = (w_qkv.shape[1] - q_cols) // 2
        norms = [v.reshape(1, width) for v in (attn_gain, attn_bias, mlp_gain, mlp_bias)]
        tabs = [t.reshape(tp, seq_rows, LANES) for t in rotary_tables(positions, head_dim)]

        parts = []
        for b in range(batch):
            cut = [(0, seq_rows // 2), (seq_rows // 2, seq_rows)] if b == 0 else [(0, seq_rows)]
            parts += [(b, lo, hi) for lo, hi in cut]
        gathered = [lax.all_gather(hidden_blk[b, lo:hi], "tp", axis=0, tiled=False) for b, lo, hi in parts]

        last_done = [positions]

        def in_turn(first, *rest):
            out = lax.optimization_barrier((first, *rest, last_done[0]))
            return out[:-1] if rest else out[0]

        expanded = [None] * batch
        for (b, lo, hi), xg in zip(parts, gathered):
            expanded[b] = expand(in_turn(xg), lo, seq_rows, norms, w_qkv, w_up_part, tabs, expanded[b])
            last_done[0] = expanded[b][1]

        me = lax.axis_index("tp")
        chip, core = me // 2, me % 2
        targets = jnp.stack([(chip + 2) % chips, (chip + 1) % chips, (chip + chips - 1) % chips, chip]).astype(jnp.int32)
        own_order = targets * 2 + core
        pair_order = targets * 2 + (1 - core)
        ring_up = lambda v: lax.ppermute(v, "tp", up_ring)
        ring_down = lambda v: lax.ppermute(v, "tp", down_ring)

        spans = []
        for b in range(batch):
            col0 = 0
            for w in [width // 2, width // 4, width // 4] if b == batch - 1 else [width]:
                spans.append((b, col0, w))
                col0 += w
        ctxs, arrived, started, merged = {}, {}, {}, {}
        result = [jnp.zeros(hidden_blk.shape, BF16)]

        def run_attend(b):
            q, kv, act = expanded[b]
            q = in_turn(q)
            ctx = attend(q.reshape(seq, q_cols), kv.reshape(seq, LANES), head_dim)
            last_done[0] = ctx
            ctxs[b] = ctx.reshape(tp, seq_rows, q_cols)

        def run_pair(i):
            b, c, w = spans[i]
            send = contract(in_turn(pair_order), ctxs[b], expanded[b][2], w_out_part, w_down_part, c, w, None)
            last_done[0] = send
            arrived[i] = lax.ppermute(send, "tp", pair)

        def run_own(i):
            b, c, w = spans[i]
            far_lo, far_hi, up_lo, up_hi, down_lo, down_hi, own = contract(
                in_turn(own_order), ctxs[b], expanded[b][2], w_out_part, w_down_part, c, w, arrived[i])
            last_done[0] = far_lo
            started[i] = (ring_up(far_lo), ring_down(far_hi), ring_up(up_hi), ring_down(down_lo), up_lo, down_hi, own)

        def run_merge(i):
            from_below, from_above, up_hi, down_lo, up_lo, down_hi, own = started[i]
            up_lo = in_turn(up_lo)
            up_lo = (up_lo + from_below.astype(F32)).astype(BF16)
            down_hi = (down_hi + from_above.astype(F32)).astype(BF16)
            last_done[0] = up_lo
            merged[i] = (ring_up(up_lo), up_hi, down_lo, ring_down(down_hi), own)

        def run_finish(i):
            b, c, w = spans[i]
            up_lo, up_hi, down_lo, down_hi, own = merged[i]
            own = in_turn(own)
            half = w // 2
            for k, (up, down) in enumerate(((up_lo, down_lo), (up_hi, down_hi))):
                lo = k * half
                total = own[:, lo:lo + half] + (up.astype(F32) + down.astype(F32))
                rows = (hidden_blk[b, :, c + lo:c + lo + half].astype(F32) + total).astype(BF16)
                result[0] = lax.dynamic_update_slice(result[0], rows[None], (b, 0, c + lo))

        for step, arg in schedule(batch, len(spans)):
            {"attend": run_attend, "pair": run_pair, "own": run_own, "merge": run_merge, "finish": run_finish}[step](arg)
        return result[0]

    return jax.shard_map(
        local_layer, mesh=mesh,
        in_specs=(P("dp", "tp", None), P(), P(), P(), P(), P(None, "tp", None), P("tp", None), P(None, "tp"), P("tp", None), P()),
        out_specs=P("dp", "tp", None), check_vma=False)
```

```python
import functools

import jax
import jax.numpy as jnp
from jax import lax
from jax.experimental import pallas as pl
from jax.experimental.pallas import tpu as pltpu
from jax.sharding import PartitionSpec as P


F32 = jnp.float32
BF16 = jnp.bfloat16
LANES = 128
ROWS = 64
VMEM_LIMIT = 67_000_000


def rotary_tables(positions, head_dim):
    inv_freq = 10000.0 ** (-2.0 * jnp.arange(head_dim // 2, dtype=F32) / head_dim)
    angles = positions.astype(F32)[:, None] * inv_freq[None, :]
    cos, sin = jnp.cos(angles), jnp.sin(angles)
    cos = jnp.concatenate([cos, cos], axis=-1)
    sin = jnp.concatenate([-sin, sin], axis=-1)
    q_tab = (jnp.concatenate([cos, cos], axis=-1), jnp.concatenate([sin, sin], axis=-1))
    kv_tab = (jnp.concatenate([cos, jnp.ones_like(cos)], axis=-1), jnp.concatenate([sin, jnp.zeros_like(sin)], axis=-1))
    return q_tab + kv_tab


def rotate(vals, cos, sin, first_half):
    half = LANES // 4
    vals = vals.astype(BF16).astype(F32)
    swapped = jnp.where(first_half, pltpu.roll(vals, LANES - half, 1), pltpu.roll(vals, half, 1))
    return (vals * cos + swapped * sin).astype(BF16)


def norm_rows(x_buf, out_buf, mean, rstd, gain, bias, start, count, width):
    at = pl.ds(start, count)
    for c in range(width // LANES):
        cols = pl.ds(c * LANES, LANES)
        n = (x_buf[at, cols].astype(F32) - mean) * rstd
        out_buf[at, cols] = (n * gain[:, cols] + bias[:, cols]).astype(BF16)


def expand_kernel(devs, width, q_tiles, up_tiles, aliased, x_hbm, mean_ref, rstd_ref, a_gain, a_bias, m_gain, m_bias, wq, wkv, wu, qc, qs, kc, ks, *refs):
    refs = refs[3:] if aliased else refs
    q_out, kv_out, act_out, x_buf, a_buf, m_buf, pend, stat, sems = refs
    m, n = pl.program_id(0), pl.program_id(1)
    rows = devs * ROWS

    def fetch(tile, d):
        return pltpu.make_async_copy(
            x_hbm.at[d, pl.ds(tile * ROWS, ROWS)], x_buf.at[pl.ds(d * ROWS, ROWS)], sems.at[d])

    def row_stats(start, count):
        at = pl.ds(start, count)
        return stat[0, at, :], stat[1, at, :]

    @pl.when((m == 0) & (n == 0))
    def _():
        for d in range(devs):
            fetch(0, d).start()

    @pl.when((n == 0) | (n == q_tiles + 2))
    def _():
        stat[0] = mean_ref[...].reshape(rows, LANES)
        stat[1] = rstd_ref[...].reshape(rows, LANES)

    @pl.when((m == 0) & (n == 0))
    def _():
        def one(d, carry):
            fetch(0, d).wait()
            start = pl.multiple_of(d * ROWS, ROWS)
            mean, rstd = row_stats(start, ROWS)
            norm_rows(x_buf, a_buf, mean, rstd, a_gain, a_bias, start, ROWS, width)
            return carry

        lax.fori_loop(0, devs, one, 0)

    @pl.when((n == q_tiles) & (m + 1 < pl.num_programs(0)))
    def _():
        for d in range(devs):
            fetch(m + 1, d).start()

    @pl.when((n == q_tiles + 2) & (m + 1 < pl.num_programs(0)))
    def _():
        for d in range(devs):
            fetch(m + 1, d).wait()

    first_half = lax.rem(lax.broadcasted_iota(jnp.int32, (rows, LANES), 1), LANES // 2) < LANES // 4

    @pl.when(n < q_tiles)
    def _():
        count = rows // q_tiles
        start = pl.multiple_of(n * count, count)
        mean, rstd = row_stats(start, count)
        norm_rows(x_buf, m_buf, mean, rstd, m_gain, m_bias, start, count, width)
        acc = jnp.dot(a_buf[...], wq[...], preferred_element_type=F32)
        cos, sin = qc[...].reshape(rows, LANES), qs[...].reshape(rows, LANES)
        for c in range(acc.shape[1] // LANES):
            part = rotate(acc[:, c * LANES:(c + 1) * LANES], cos, sin, first_half)
            q_out[:, :, pl.ds(c * LANES, LANES)] = part.reshape(devs, ROWS, LANES)

    @pl.when(n == q_tiles)
    def _():
        acc = jnp.dot(a_buf[...], wkv[...], preferred_element_type=F32)
        cos, sin = kc[...].reshape(rows, LANES), ks[...].reshape(rows, LANES)
        kv_out[...] = rotate(acc, cos, sin, first_half).reshape(devs, ROWS, LANES)

    def gelu_out():
        u = pend[...]
        act = 0.5 * u * (1.0 + lax.erf(u * 0.7071067811865476))
        act_out[...] = act.astype(BF16).reshape(devs, ROWS, act.shape[1])

    def up_dot():
        pend[...] = jnp.dot(m_buf[...], wu[...], preferred_element_type=F32)

    @pl.when(n == q_tiles + 1)
    def _():
        up_dot()

    @pl.when((n > q_tiles + 1) & (n <= q_tiles + up_tiles))
    def _():
        count = pl.cdiv(pl.cdiv(rows, up_tiles - 1), 16) * 16
        start = pl.multiple_of(jnp.minimum((n - q_tiles - 2) * count, rows - count), 16)
        mean, rstd = row_stats(start, count)
        norm_rows(x_buf, a_buf, mean, rstd, a_gain, a_bias, start, count, width)
        gelu_out()
        up_dot()

    @pl.when(n == q_tiles + up_tiles + 1)
    def _():
        gelu_out()


def expand(xg, batch_id, row0, seq_rows, stats, norms, w_qkv, w_up, tabs, prev):
    devs, chunk, width = xg.shape
    q_cols = w_qkv.shape[1] - LANES
    up_cols = w_up.shape[1]
    tq, tu = min(256, q_cols), min(512, up_cols)
    q_tiles, up_tiles = q_cols // tq, up_cols // tu
    m_tiles = chunk // ROWS
    h0 = row0 // ROWS
    rows = devs * ROWS
    vec = pl.BlockSpec((1, width), lambda m, n: (0, 0))
    tab = pl.BlockSpec((devs, ROWS, LANES), lambda m, n: (0, h0 + m, 0))
    any_spec = pl.BlockSpec(memory_space=pl.ANY)
    stat_specs = [
        pl.BlockSpec((None, None, devs, ROWS, LANES), lambda m, n, k=k: (
            k, batch_id, 0, h0 + jnp.minimum(m + (n > q_tiles).astype(jnp.int32), m_tiles - 1), 0))
        for k in range(2)
    ]
    in_specs = [
        any_spec, *stat_specs, vec, vec, vec, vec,
        pl.BlockSpec((width, tq), lambda m, n: (0, jnp.minimum(n, q_tiles - 1))),
        pl.BlockSpec((width, LANES), lambda m, n: (0, q_cols // LANES)),
        pl.BlockSpec((width, tu), lambda m, n: (0, jnp.clip(n - q_tiles - 1, 0, up_tiles - 1))),
        tab, tab, tab, tab,
    ]
    args = [xg, stats, stats, *norms, w_qkv, w_qkv, w_up, *tabs]
    aliases = {}
    if prev is not None:
        aliases = {len(args) + k: k for k in range(3)}
        in_specs += [any_spec] * 3
        args += list(prev)
    out_shape = [jax.ShapeDtypeStruct((devs, seq_rows, c), BF16) for c in (q_cols, LANES, up_cols)]
    out_specs = [
        pl.BlockSpec((devs, ROWS, tq), lambda m, n: (0, h0 + m, jnp.minimum(n, q_tiles - 1))),
        pl.BlockSpec((devs, ROWS, LANES), lambda m, n: (0, h0 + m, 0)),
        pl.BlockSpec((devs, ROWS, tu), lambda m, n: (0, h0 + m, jnp.clip(n - q_tiles - 2, 0, up_tiles - 1))),
    ]
    flops = 2 * devs * chunk * width * (q_cols + LANES + up_cols)
    return pl.pallas_call(
        functools.partial(expand_kernel, devs, width, q_tiles, up_tiles, prev is not None),
        grid=(m_tiles, q_tiles + up_tiles + 2),
        in_specs=in_specs,
        out_specs=out_specs,
        out_shape=out_shape,
        scratch_shapes=[
            pltpu.VMEM((rows, width), BF16), pltpu.VMEM((rows, width), BF16), pltpu.VMEM((rows, width), BF16),
            pltpu.VMEM((rows, tu), F32), pltpu.VMEM((2, rows, LANES), F32), pltpu.SemaphoreType.DMA((devs,)),
        ],
        input_output_aliases=aliases,
        compiler_params=pltpu.CompilerParams(vmem_limit_bytes=VMEM_LIMIT),
        cost_estimate=pl.CostEstimate(flops=flops, bytes_accessed=2 * width * (q_cols + up_cols), transcendentals=0),
        name="expand",
    )(*args)


def attend_kernel(seq, head_dim, q_ref, kv_ref, out_ref, k_lo, k_hi, v_lo, v_hi):
    scale = head_dim ** -0.5

    @pl.when(pl.program_id(0) == 0)
    def _():
        kv = kv_ref[...].astype(F32)
        low = lax.broadcasted_iota(jnp.int32, kv.shape, 1) < head_dim
        keys = jnp.where(low, kv, 0.0)
        vals = jnp.where(low, 0.0, kv)
        k_lo[...] = keys.astype(BF16)
        k_hi[...] = pltpu.roll(keys, head_dim, 1).astype(BF16)
        v_hi[...] = vals.astype(BF16)
        v_lo[...] = pltpu.roll(vals, head_dim, 1).astype(BF16)

    blk = min(256, seq)
    row = lax.broadcasted_iota(jnp.int32, (blk, blk), 0)
    col = lax.broadcasted_iota(jnp.int32, (blk, blk), 1)
    allowed = col <= row
    for b in range(seq // blk):
        q = q_ref[pl.ds(b * blk, blk), :]
        keys = (b + 1) * blk
        ctx = None
        for k_ref, v_ref in ((k_lo, v_lo), (k_hi, v_hi)):
            s = lax.dot_general(q, k_ref[pl.ds(0, keys), :], (((1,), (1,)), ((), ())), preferred_element_type=F32)
            diag = jnp.where(allowed, s[:, b * blk:], -1e30)
            s = diag if b == 0 else jnp.concatenate([s[:, :b * blk], diag], axis=1)
            e = jnp.exp((s - jnp.max(s, axis=-1, keepdims=True)) * scale)
            p = (e * (1.0 / jnp.sum(e, axis=-1, keepdims=True))).astype(BF16)
            part = jnp.dot(p, v_ref[pl.ds(0, keys), :], preferred_element_type=F32)
            ctx = part if ctx is None else ctx + part
        out_ref[pl.ds(b * blk, blk), :] = ctx.astype(BF16)


def attend(q, kv, head_dim):
    seq, q_cols = q.shape
    flops = 2 * seq * seq * q_cols * 4
    return pl.pallas_call(
        functools.partial(attend_kernel, seq, head_dim),
        grid=(q_cols // LANES,),
        in_specs=[pl.BlockSpec((seq, LANES), lambda h: (0, h)), pl.BlockSpec((seq, LANES), lambda h: (0, 0))],
        out_specs=pl.BlockSpec((seq, LANES), lambda h: (0, h)),
        out_shape=jax.ShapeDtypeStruct((seq, q_cols), BF16),
        scratch_shapes=[pltpu.VMEM((seq, LANES), BF16)] * 4,
        compiler_params=pltpu.CompilerParams(vmem_limit_bytes=VMEM_LIMIT),
        cost_estimate=pl.CostEstimate(flops=flops, bytes_accessed=4 * seq * q_cols, transcendentals=0),
        name="attend",
    )(q, kv)


def contract_kernel(num, final, j0, steps, tn, order, ctx_hbm, act_hbm, wo_hbm, wd_hbm, *refs):
    refs, (ctx_buf, act_buf, sem) = refs[:-3], refs[-3:]
    blk = ctx_hbm.shape[1]
    cps = []
    for k in range(num):
        rows = pl.ds(k * blk, blk)
        cps.append(pltpu.make_async_copy(act_hbm.at[order[k]], act_buf.at[rows], sem))
        cps.append(pltpu.make_async_copy(ctx_hbm.at[order[k]], ctx_buf.at[rows], sem))
    for cp in cps:
        cp.start()

    def product(j, wo, wd):
        @pl.when(j == 0)
        def _():
            for cp in cps:
                cp.wait()

        acc = jnp.dot(act_buf[...], wd[...], preferred_element_type=F32)
        acc = acc + jnp.dot(ctx_buf[...], wo[...], preferred_element_type=F32)
        return acc.reshape(num, blk, tn)

    def pair_body(wo, wd, send):
        send[...] = product(pl.program_id(0), wo, wd).astype(BF16)

    def own_body(wo, wd, add, far_lo, far_hi, up, down, up_lo, down_hi, own):
        j = pl.program_id(0)
        acc = product(j, wo, wd) + add[...].astype(F32)
        own[...] = acc[3]
        up[...] = acc[1].astype(BF16)
        down[...] = acc[2].astype(BF16)

        @pl.when(j < steps // 2)
        def _():
            far_lo[...] = acc[0].astype(BF16)
            up_lo[...] = acc[1]

        @pl.when(j >= steps // 2)
        def _():
            far_hi[...] = acc[0].astype(BF16)
            down_hi[...] = acc[2]

    weights = [pl.BlockSpec((w.shape[0], tn), lambda j: (0, j0 + j)) for w in (wo_hbm, wd_hbm)]
    block = pl.BlockSpec((num, blk, tn), lambda j: (0, 0, j))
    one = pl.BlockSpec((blk, tn), lambda j: (0, j))
    lo = pl.BlockSpec((blk, tn), lambda j: (0, jnp.minimum(j, steps // 2 - 1)))
    hi = pl.BlockSpec((blk, tn), lambda j: (0, jnp.maximum(j - steps // 2, 0)))
    if final:
        pltpu.emit_pipeline(own_body, grid=(steps,), in_specs=weights + [pl.BlockSpec((num, blk, tn), lambda j: (0, 0, final[0] + j))],
                            out_specs=[lo, hi, one, one, lo, hi, one])(wo_hbm, wd_hbm, *refs)
    else:
        pltpu.emit_pipeline(pair_body, grid=(steps,), in_specs=weights, out_specs=[block])(wo_hbm, wd_hbm, *refs)


def contract(order, ctx, act, w_out, w_down, col0, cols, add=None, add_col0=0):
    num = order.shape[0]
    _, blk, _ = ctx.shape
    tn = min(512, cols // 2)
    steps = cols // tn
    any_spec = pl.BlockSpec(memory_space=pl.ANY)
    args = [order, ctx, act, w_out, w_down]
    if add is not None:
        args.append(add)
        half, full = (lambda t: jax.ShapeDtypeStruct((blk, cols // 2), t)), (lambda t: jax.ShapeDtypeStruct((blk, cols), t))
        out_shape = [half(BF16), half(BF16), full(BF16), full(BF16), half(F32), half(F32), full(F32)]
    else:
        out_shape = [jax.ShapeDtypeStruct((num, blk, cols), BF16)]
    depth = w_out.shape[0] + w_down.shape[0]
    return pl.pallas_call(
        functools.partial(contract_kernel, num, None if add is None else (add_col0 // tn,), col0 // tn, steps, tn),
        in_specs=[pl.BlockSpec(memory_space=pltpu.SMEM)] + [any_spec] * (len(args) - 1),
        out_specs=[any_spec] * len(out_shape),
        out_shape=out_shape,
        scratch_shapes=[
            pltpu.VMEM((num * blk, w_out.shape[0]), BF16), pltpu.VMEM((num * blk, w_down.shape[0]), BF16),
            pltpu.SemaphoreType.DMA,
        ],
        compiler_params=pltpu.CompilerParams(vmem_limit_bytes=VMEM_LIMIT),
        cost_estimate=pl.CostEstimate(flops=2 * num * blk * cols * depth, bytes_accessed=2 * depth * cols, transcendentals=0),
        name="contract_pair" if add is None else "contract_own",
    )(*args)


def merge_kernel(up_lo, down_hi, below, above, up_any, down_any, up, down):
    up[...] = (up_lo[...] + below[...].astype(F32)).astype(BF16)
    down[...] = (down_hi[...] + above[...].astype(F32)).astype(BF16)


def merge(up_lo, down_hi, below, above, up, down):
    blk, half = up_lo.shape
    cw = min(1024, half)
    any_spec = pl.BlockSpec(memory_space=pl.ANY)
    part = pl.BlockSpec((blk, cw), lambda j: (0, j))
    return pl.pallas_call(
        merge_kernel,
        grid=(half // cw,),
        in_specs=[part] * 4 + [any_spec] * 2,
        out_specs=[part, pl.BlockSpec((blk, cw), lambda j: (0, half // cw + j))],
        out_shape=[jax.ShapeDtypeStruct(up.shape, BF16)] * 2,
        input_output_aliases={4: 0, 5: 1},
        compiler_params=pltpu.CompilerParams(vmem_limit_bytes=VMEM_LIMIT),
        cost_estimate=pl.CostEstimate(flops=16 * blk * half, bytes_accessed=16 * blk * half, transcendentals=0),
        name="merge",
    )(up_lo, down_hi, below, above, up, down)


def finish_kernel(x, own, below, above, *refs):
    y = refs[-1]
    total = own[...] + (below[...].astype(F32) + above[...].astype(F32))
    y[...] = (x[...].astype(F32) + total).astype(BF16)


def finish(hidden, batch_id, col0, own, below, above, result):
    blk, cols = own.shape
    cw = min(1024, cols)
    j0 = col0 // cw
    part = pl.BlockSpec((blk, cw), lambda j: (0, j))
    wide = pl.BlockSpec((None, blk, cw), lambda j: (batch_id, 0, j0 + j))
    args, in_specs, aliases = [hidden, own, below, above], [wide, part, part, part], {}
    if result is not None:
        args.append(result)
        in_specs.append(pl.BlockSpec(memory_space=pl.ANY))
        aliases = {4: 0}
    return pl.pallas_call(
        finish_kernel,
        grid=(cols // cw,),
        in_specs=in_specs,
        out_specs=wide,
        out_shape=jax.ShapeDtypeStruct(hidden.shape, BF16),
        input_output_aliases=aliases,
        compiler_params=pltpu.CompilerParams(vmem_limit_bytes=VMEM_LIMIT),
        cost_estimate=pl.CostEstimate(flops=16 * blk * cols, bytes_accessed=12 * blk * cols, transcendentals=0),
        name="finish",
    )(*args)


def solution(mesh):
    tp = mesh.shape["tp"]
    chips = tp // 2
    assert tp == 2 * chips and chips == 4
    pair = [(i, i ^ 1) for i in range(tp)]
    up_ring = [(i, (i + 2) % tp) for i in range(tp)]
    down_ring = [(i, (i - 2) % tp) for i in range(tp)]

    def layer(hidden_blk, attn_gain, attn_bias, mlp_gain, mlp_bias, w_qkv_part, w_out_part, w_up_part, w_down_part, positions):
        batch, seq_rows, width = hidden_blk.shape
        seq = seq_rows * tp
        w_qkv = w_qkv_part.reshape(width, w_qkv_part.shape[2])
        q_cols = w_out_part.shape[0]
        head_dim = (w_qkv.shape[1] - q_cols) // 2
        norms = [v.reshape(1, width) for v in (attn_gain, attn_bias, mlp_gain, mlp_bias)]
        tabs = [t.reshape(tp, seq_rows, LANES) for t in rotary_tables(positions, head_dim)]

        parts = []
        for b in range(batch):
            cut = [(0, seq_rows // 2), (seq_rows // 2, seq_rows)] if b == 0 else [(0, seq_rows)]
            parts += [(b, lo, hi) for lo, hi in cut]
        gathered = [lax.all_gather(hidden_blk[b, lo:hi], "tp", axis=0, tiled=False) for b, lo, hi in parts]

        last_done, result = [positions], [None]

        def in_turn(first):
            out = lax.optimization_barrier((first, last_done[0]))
            if last_done[0] is result:
                result[0] = out[1][0]
            return out[0]

        x32 = hidden_blk.astype(F32)
        mean = jnp.mean(x32, axis=-1, keepdims=True)
        centered = x32 - mean
        rstd = lax.rsqrt(jnp.mean(centered * centered, axis=-1, keepdims=True) + 1e-5)
        stats = lax.all_gather(jnp.stack([mean[..., 0], rstd[..., 0]]), "tp", axis=2, tiled=False)
        stats = jnp.broadcast_to(stats[..., None], (2, batch, tp, seq_rows, LANES))

        expanded = [None] * batch

        def run_expand(b):
            for (pb, lo, hi), xg in zip(parts, gathered):
                if pb == b:
                    expanded[b] = expand(in_turn(xg), b, lo, seq_rows, stats, norms, w_qkv, w_up_part, tabs, expanded[b])
                    last_done[0] = expanded[b][1]

        me = lax.axis_index("tp")
        chip, core = me // 2, me % 2
        targets = jnp.stack([(chip + 2) % chips, (chip + 1) % chips, (chip + chips - 1) % chips, chip]).astype(jnp.int32)
        own_order = targets * 2 + core
        pair_order = targets * 2 + (1 - core)
        ring_up = lambda v: lax.ppermute(v, "tp", up_ring)
        ring_down = lambda v: lax.ppermute(v, "tp", down_ring)

        ctxs, arrived, started, merged = {}, {}, {}, {}

        def run_attend(b):
            q, kv, _ = expanded[b]
            q = in_turn(q)
            ctx = attend(q.reshape(seq, q_cols), kv.reshape(seq, LANES), head_dim)
            last_done[0] = ctx
            ctxs[b] = ctx.reshape(tp, seq_rows, q_cols)

        def run_pair(span):
            b, c, w = span
            (send,) = contract(in_turn(pair_order), ctxs[b], expanded[b][2], w_out_part, w_down_part, c, w)
            last_done[0] = send
            arrived[span] = lax.ppermute(send, "tp", pair)

        def run_own(span):
            b, c, w = span
            pb, pc, pw = next(p for p in arrived if p[0] == b and p[1] <= c and c + w <= p[1] + p[2])
            far_lo, far_hi, up, down, up_lo, down_hi, own = contract(
                in_turn(own_order), ctxs[b], expanded[b][2], w_out_part, w_down_part, c, w, arrived[pb, pc, pw], c - pc)
            last_done[0] = far_lo
            started[span] = (up_lo, down_hi, ring_up(far_lo), ring_down(far_hi), up, down, own)

        def run_merge(span):
            up_lo, down_hi, below, above, up, down, own = started[span]
            up, down = merge(in_turn(up_lo), down_hi, below, above, up, down)
            last_done[0] = up
            merged[span] = (own, ring_up(up), ring_down(down))

        def run_finish(span):
            own, below, above = merged[span]
            result[0] = finish(hidden_blk, span[0], span[1], in_turn(own), below, above, result[0])
            last_done[0] = result

        whole = [(b, 0, width) for b in range(batch)]
        last, half, quarter = batch - 1, width // 2, width // 4
        pairs = [(last, 0, half), (last, half, half)]
        ends = [(last, 0, half), (last, half, quarter), (last, half + quarter, quarter)]
        run_expand(0)
        run_attend(0)
        run_pair(whole[0])
        for b in range(1, batch):
            run_expand(b)
            if b >= 2:
                run_finish(whole[b - 2])
            run_own(whole[b - 1])
            run_attend(b)
            if b < last:
                run_pair(whole[b])
            run_merge(whole[b - 1])
        run_pair(pairs[0])
        run_pair(pairs[1])
        run_own(ends[0])
        run_finish(whole[last - 1])
        run_own(ends[1])
        run_merge(ends[0])
        run_own(ends[2])
        run_merge(ends[1])
        run_finish(ends[0])
        run_merge(ends[2])
        run_finish(ends[1])
        run_finish(ends[2])
        return result[0]

    return jax.shard_map(
        layer, mesh=mesh,
        in_specs=(P("dp", "tp", None), P(), P(), P(), P(), P(None, "tp", None), P("tp", None), P(None, "tp"), P("tp", None), P()),
        out_specs=P("dp", "tp", None), check_vma=False)
```

```python
import functools

import jax
import jax.numpy as jnp
from jax import lax
from jax.experimental import pallas as pl
from jax.experimental.pallas import tpu as pltpu
from jax.sharding import PartitionSpec as P


F32 = jnp.float32
BF16 = jnp.bfloat16
LANES = 128
ROWS = 64
VMEM_LIMIT = 67_000_000


def rotary_tables(positions, head_dim):
    inv_freq = 10000.0 ** (-2.0 * jnp.arange(head_dim // 2, dtype=F32) / head_dim)
    angles = positions.astype(F32)[:, None] * inv_freq[None, :]
    cos, sin = jnp.cos(angles), jnp.sin(angles)
    cos = jnp.concatenate([cos, cos], axis=-1)
    sin = jnp.concatenate([-sin, sin], axis=-1)
    q_tab = (jnp.concatenate([cos, cos], axis=-1), jnp.concatenate([sin, sin], axis=-1))
    kv_tab = (jnp.concatenate([cos, jnp.ones_like(cos)], axis=-1), jnp.concatenate([sin, jnp.zeros_like(sin)], axis=-1))
    return q_tab + kv_tab


def rotate(vals, cos, sin, first_half):
    half = LANES // 4
    vals = vals.astype(BF16).astype(F32)
    swapped = jnp.where(first_half, pltpu.roll(vals, LANES - half, 1), pltpu.roll(vals, half, 1))
    return (vals * cos + swapped * sin).astype(BF16)


def norm_rows(x_buf, out_buf, mean, rstd, gain, bias, start, count, col0, cols):
    at = pl.ds(start, count)
    for c in range(col0, col0 + cols, LANES):
        lanes = pl.ds(c, LANES)
        n = (x_buf[at, lanes].astype(F32) - mean) * rstd
        out_buf[at, lanes] = (n * gain[:, lanes] + bias[:, lanes]).astype(BF16)


def dot_beside(acc, lhs, rhs, width, pieces, beside):
    depth = width // pieces
    for k in range(pieces):
        beside(k * depth, depth)
        part = jnp.dot(lhs[:, pl.ds(k * depth, depth)], rhs[pl.ds(k * depth, depth), :], preferred_element_type=F32)
        acc[...] = part if k == 0 else acc[...] + part


def expand_kernel(devs, width, q_tiles, up_tiles, aliased, x_hbm, mean_ref, rstd_ref, a_gain, a_bias, m_gain, m_bias, wq, wkv, wu, qc, qs, kc, ks, *refs):
    refs = refs[3:] if aliased else refs
    q_out, kv_out, act_out, x_buf, a_buf, m_buf, pend, q_acc, stat, sems = refs
    m, n = pl.program_id(0), pl.program_id(1)
    rows = devs * ROWS

    def fetch(tile, d):
        return pltpu.make_async_copy(
            x_hbm.at[d, pl.ds(tile * ROWS, ROWS)], x_buf.at[pl.ds(d * ROWS, ROWS)], sems.at[d])

    def row_stats(start, count):
        at = pl.ds(start, count)
        return stat[0, at, :], stat[1, at, :]

    @pl.when((m == 0) & (n == 0))
    def _():
        for d in range(devs):
            fetch(0, d).start()

    @pl.when((n == 0) | (n == q_tiles + 2))
    def _():
        stat[0] = mean_ref[...].reshape(rows, LANES)
        stat[1] = rstd_ref[...].reshape(rows, LANES)

    @pl.when((m == 0) & (n == 0))
    def _():
        def one(d, carry):
            fetch(0, d).wait()
            start = pl.multiple_of(d * ROWS, ROWS)
            mean, rstd = row_stats(start, ROWS)
            norm_rows(x_buf, a_buf, mean, rstd, a_gain, a_bias, start, ROWS, 0, width)
            return carry

        lax.fori_loop(0, devs, one, 0)

    @pl.when((n == q_tiles) & (m + 1 < pl.num_programs(0)))
    def _():
        for d in range(devs):
            fetch(m + 1, d).start()

    @pl.when((n == q_tiles + 2) & (m + 1 < pl.num_programs(0)))
    def _():
        for d in range(devs):
            fetch(m + 1, d).wait()

    first_half = lax.rem(lax.broadcasted_iota(jnp.int32, (rows, LANES), 1), LANES // 2) < LANES // 4

    @pl.when(n < q_tiles)
    def _():
        count = rows // q_tiles
        start = pl.multiple_of(n * count, count)
        mean, rstd = row_stats(start, count)
        dot_beside(q_acc, a_buf, wq, width, 16, lambda col0, cols: norm_rows(
            x_buf, m_buf, mean, rstd, m_gain, m_bias, start, count, col0, cols))
        acc = q_acc[...]
        cos, sin = qc[...].reshape(rows, LANES), qs[...].reshape(rows, LANES)
        for c in range(acc.shape[1] // LANES):
            part = rotate(acc[:, c * LANES:(c + 1) * LANES], cos, sin, first_half)
            q_out[:, :, pl.ds(c * LANES, LANES)] = part.reshape(devs, ROWS, LANES)

    @pl.when(n == q_tiles)
    def _():
        acc = jnp.dot(a_buf[...], wkv[...], preferred_element_type=F32)
        cos, sin = kc[...].reshape(rows, LANES), ks[...].reshape(rows, LANES)
        kv_out[...] = rotate(acc, cos, sin, first_half).reshape(devs, ROWS, LANES)

    def gelu_out():
        u = pend[...]
        act = 0.5 * u * (1.0 + lax.erf(u * 0.7071067811865476))
        act_out[...] = act.astype(BF16).reshape(devs, ROWS, act.shape[1])

    def up_dot():
        pend[...] = jnp.dot(m_buf[...], wu[...], preferred_element_type=F32)

    @pl.when(n == q_tiles + 1)
    def _():
        up_dot()

    @pl.when((n > q_tiles + 1) & (n <= q_tiles + up_tiles))
    def _():
        count = pl.cdiv(pl.cdiv(rows, up_tiles - 1), 16) * 16
        start = pl.multiple_of(jnp.minimum((n - q_tiles - 2) * count, rows - count), 16)
        mean, rstd = row_stats(start, count)
        gelu_out()
        dot_beside(pend, m_buf, wu, width, 8, lambda col0, cols: norm_rows(
            x_buf, a_buf, mean, rstd, a_gain, a_bias, start, count, col0, cols))

    @pl.when(n == q_tiles + up_tiles + 1)
    def _():
        gelu_out()


def expand(xg, batch_id, row0, seq_rows, stats, norms, w_qkv, w_up, tabs, prev):
    devs, chunk, width = xg.shape
    q_cols = w_qkv.shape[1] - LANES
    up_cols = w_up.shape[1]
    tq, tu = min(256, q_cols), min(512, up_cols)
    q_tiles, up_tiles = q_cols // tq, up_cols // tu
    m_tiles = chunk // ROWS
    h0 = row0 // ROWS
    rows = devs * ROWS
    vec = pl.BlockSpec((1, width), lambda m, n: (0, 0))
    tab = pl.BlockSpec((devs, ROWS, LANES), lambda m, n: (0, h0 + m, 0))
    any_spec = pl.BlockSpec(memory_space=pl.ANY)
    stat_specs = [
        pl.BlockSpec((None, None, devs, ROWS, LANES), lambda m, n, k=k: (
            k, batch_id, 0, h0 + jnp.minimum(m + (n > q_tiles).astype(jnp.int32), m_tiles - 1), 0))
        for k in range(2)
    ]
    in_specs = [
        any_spec, *stat_specs, vec, vec, vec, vec,
        pl.BlockSpec((width, tq), lambda m, n: (0, jnp.minimum(n, q_tiles - 1))),
        pl.BlockSpec((width, LANES), lambda m, n: (0, q_cols // LANES)),
        pl.BlockSpec((width, tu), lambda m, n: (0, jnp.clip(n - q_tiles - 1, 0, up_tiles - 1))),
        tab, tab, tab, tab,
    ]
    args = [xg, stats, stats, *norms, w_qkv, w_qkv, w_up, *tabs]
    aliases = {}
    if prev is not None:
        aliases = {len(args) + k: k for k in range(3)}
        in_specs += [any_spec] * 3
        args += list(prev)
    out_shape = [jax.ShapeDtypeStruct((devs, seq_rows, c), BF16) for c in (q_cols, LANES, up_cols)]
    out_specs = [
        pl.BlockSpec((devs, ROWS, tq), lambda m, n: (0, h0 + m, jnp.minimum(n, q_tiles - 1))),
        pl.BlockSpec((devs, ROWS, LANES), lambda m, n: (0, h0 + m, 0)),
        pl.BlockSpec((devs, ROWS, tu), lambda m, n: (0, h0 + m, jnp.clip(n - q_tiles - 2, 0, up_tiles - 1))),
    ]
    flops = 2 * devs * chunk * width * (q_cols + LANES + up_cols)
    return pl.pallas_call(
        functools.partial(expand_kernel, devs, width, q_tiles, up_tiles, prev is not None),
        grid=(m_tiles, q_tiles + up_tiles + 2),
        in_specs=in_specs,
        out_specs=out_specs,
        out_shape=out_shape,
        scratch_shapes=[
            pltpu.VMEM((rows, width), BF16), pltpu.VMEM((rows, width), BF16), pltpu.VMEM((rows, width), BF16),
            pltpu.VMEM((rows, tu), F32), pltpu.VMEM((rows, tq), F32), pltpu.VMEM((2, rows, LANES), F32), pltpu.SemaphoreType.DMA((devs,)),
        ],
        input_output_aliases=aliases,
        compiler_params=pltpu.CompilerParams(vmem_limit_bytes=VMEM_LIMIT),
        cost_estimate=pl.CostEstimate(flops=flops, bytes_accessed=2 * width * (q_cols + up_cols), transcendentals=0),
        name="expand",
    )(*args)


def attend_kernel(seq, head_dim, q_ref, kv_ref, out_ref, k_lo, k_hi, v_lo, v_hi):
    scale = head_dim ** -0.5

    @pl.when(pl.program_id(0) == 0)
    def _():
        kv = kv_ref[...].astype(F32)
        low = lax.broadcasted_iota(jnp.int32, kv.shape, 1) < head_dim
        keys = jnp.where(low, kv, 0.0)
        vals = jnp.where(low, 0.0, kv)
        k_lo[...] = keys.astype(BF16)
        k_hi[...] = pltpu.roll(keys, head_dim, 1).astype(BF16)
        v_hi[...] = vals.astype(BF16)
        v_lo[...] = pltpu.roll(vals, head_dim, 1).astype(BF16)

    blk = min(256, seq)
    row = lax.broadcasted_iota(jnp.int32, (blk, blk), 0)
    col = lax.broadcasted_iota(jnp.int32, (blk, blk), 1)
    allowed = col <= row
    for b in range(seq // blk):
        q = q_ref[pl.ds(b * blk, blk), :]
        keys = (b + 1) * blk
        ctx = None
        for k_ref, v_ref in ((k_lo, v_lo), (k_hi, v_hi)):
            s = lax.dot_general(q, k_ref[pl.ds(0, keys), :], (((1,), (1,)), ((), ())), preferred_element_type=F32)
            diag = jnp.where(allowed, s[:, b * blk:], -1e30)
            s = diag if b == 0 else jnp.concatenate([s[:, :b * blk], diag], axis=1)
            e = jnp.exp((s - jnp.max(s, axis=-1, keepdims=True)) * scale)
            p = (e * (1.0 / jnp.sum(e, axis=-1, keepdims=True))).astype(BF16)
            part = jnp.dot(p, v_ref[pl.ds(0, keys), :], preferred_element_type=F32)
            ctx = part if ctx is None else ctx + part
        out_ref[pl.ds(b * blk, blk), :] = ctx.astype(BF16)


def attend(q, kv, head_dim):
    seq, q_cols = q.shape
    flops = 2 * seq * seq * q_cols * 4
    return pl.pallas_call(
        functools.partial(attend_kernel, seq, head_dim),
        grid=(q_cols // LANES,),
        in_specs=[pl.BlockSpec((seq, LANES), lambda h: (0, h)), pl.BlockSpec((seq, LANES), lambda h: (0, 0))],
        out_specs=pl.BlockSpec((seq, LANES), lambda h: (0, h)),
        out_shape=jax.ShapeDtypeStruct((seq, q_cols), BF16),
        scratch_shapes=[pltpu.VMEM((seq, LANES), BF16)] * 4,
        compiler_params=pltpu.CompilerParams(vmem_limit_bytes=VMEM_LIMIT),
        cost_estimate=pl.CostEstimate(flops=flops, bytes_accessed=4 * seq * q_cols, transcendentals=0),
        name="attend",
    )(q, kv)


def contract_kernel(num, final, j0, steps, tn, order, ctx_hbm, act_hbm, wo_hbm, wd_hbm, *refs):
    refs, (ctx_buf, act_buf, sem) = refs[:-3], refs[-3:]
    blk = ctx_hbm.shape[1]
    cps = []
    for k in range(num):
        rows = pl.ds(k * blk, blk)
        cps.append(pltpu.make_async_copy(act_hbm.at[order[k]], act_buf.at[rows], sem))
        cps.append(pltpu.make_async_copy(ctx_hbm.at[order[k]], ctx_buf.at[rows], sem))
    for cp in cps:
        cp.start()

    def product(j, wo, wd):
        @pl.when(j == 0)
        def _():
            for cp in cps:
                cp.wait()

        acc = jnp.dot(act_buf[...], wd[...], preferred_element_type=F32)
        acc = acc + jnp.dot(ctx_buf[...], wo[...], preferred_element_type=F32)
        return acc.reshape(num, blk, tn)

    def pair_body(wo, wd, send):
        send[...] = product(pl.program_id(0), wo, wd).astype(BF16)

    def own_body(wo, wd, add, far_lo, far_hi, up, down, up_lo, down_hi, own):
        j = pl.program_id(0)
        acc = product(j, wo, wd) + add[...].astype(F32)
        own[...] = acc[3]
        up[...] = acc[1].astype(BF16)
        down[...] = acc[2].astype(BF16)

        @pl.when(j < steps // 2)
        def _():
            far_lo[...] = acc[0].astype(BF16)
            up_lo[...] = acc[1]

        @pl.when(j >= steps // 2)
        def _():
            far_hi[...] = acc[0].astype(BF16)
            down_hi[...] = acc[2]

    weights = [pl.BlockSpec((w.shape[0], tn), lambda j: (0, j0 + j)) for w in (wo_hbm, wd_hbm)]
    block = pl.BlockSpec((num, blk, tn), lambda j: (0, 0, j))
    one = pl.BlockSpec((blk, tn), lambda j: (0, j))
    lo = pl.BlockSpec((blk, tn), lambda j: (0, jnp.minimum(j, steps // 2 - 1)))
    hi = pl.BlockSpec((blk, tn), lambda j: (0, jnp.maximum(j - steps // 2, 0)))
    if final:
        pltpu.emit_pipeline(own_body, grid=(steps,), in_specs=weights + [pl.BlockSpec((num, blk, tn), lambda j: (0, 0, final[0] + j))],
                            out_specs=[lo, hi, one, one, lo, hi, one])(wo_hbm, wd_hbm, *refs)
    else:
        pltpu.emit_pipeline(pair_body, grid=(steps,), in_specs=weights, out_specs=[block])(wo_hbm, wd_hbm, *refs)


def contract(order, ctx, act, w_out, w_down, col0, cols, add=None, add_col0=0):
    num = order.shape[0]
    _, blk, _ = ctx.shape
    tn = min(512, cols // 2)
    steps = cols // tn
    any_spec = pl.BlockSpec(memory_space=pl.ANY)
    args = [order, ctx, act, w_out, w_down]
    if add is not None:
        args.append(add)
        half, full = (lambda t: jax.ShapeDtypeStruct((blk, cols // 2), t)), (lambda t: jax.ShapeDtypeStruct((blk, cols), t))
        out_shape = [half(BF16), half(BF16), full(BF16), full(BF16), half(F32), half(F32), full(F32)]
    else:
        out_shape = [jax.ShapeDtypeStruct((num, blk, cols), BF16)]
    depth = w_out.shape[0] + w_down.shape[0]
    return pl.pallas_call(
        functools.partial(contract_kernel, num, None if add is None else (add_col0 // tn,), col0 // tn, steps, tn),
        in_specs=[pl.BlockSpec(memory_space=pltpu.SMEM)] + [any_spec] * (len(args) - 1),
        out_specs=[any_spec] * len(out_shape),
        out_shape=out_shape,
        scratch_shapes=[
            pltpu.VMEM((num * blk, w_out.shape[0]), BF16), pltpu.VMEM((num * blk, w_down.shape[0]), BF16),
            pltpu.SemaphoreType.DMA,
        ],
        compiler_params=pltpu.CompilerParams(vmem_limit_bytes=VMEM_LIMIT),
        cost_estimate=pl.CostEstimate(flops=2 * num * blk * cols * depth, bytes_accessed=2 * depth * cols, transcendentals=0),
        name="contract_pair" if add is None else "contract_own",
    )(*args)


def merge_kernel(up_lo, down_hi, below, above, up_any, down_any, up, down):
    up[...] = (up_lo[...] + below[...].astype(F32)).astype(BF16)
    down[...] = (down_hi[...] + above[...].astype(F32)).astype(BF16)


def merge(up_lo, down_hi, below, above, up, down):
    blk, half = up_lo.shape
    cw = min(2048, half)
    any_spec = pl.BlockSpec(memory_space=pl.ANY)
    part = pl.BlockSpec((blk, cw), lambda j: (0, j))
    return pl.pallas_call(
        merge_kernel,
        grid=(half // cw,),
        in_specs=[part] * 4 + [any_spec] * 2,
        out_specs=[part, pl.BlockSpec((blk, cw), lambda j: (0, half // cw + j))],
        out_shape=[jax.ShapeDtypeStruct(up.shape, BF16)] * 2,
        input_output_aliases={4: 0, 5: 1},
        compiler_params=pltpu.CompilerParams(vmem_limit_bytes=VMEM_LIMIT),
        cost_estimate=pl.CostEstimate(flops=16 * blk * half, bytes_accessed=16 * blk * half, transcendentals=0),
        name="merge",
    )(up_lo, down_hi, below, above, up, down)


def finish_kernel(x, own, below, above, *refs):
    y = refs[-1]
    total = own[...] + (below[...].astype(F32) + above[...].astype(F32))
    y[...] = (x[...].astype(F32) + total).astype(BF16)


def finish(hidden, batch_id, col0, own, below, above, result):
    blk, cols = own.shape
    cw = min(2048, cols)
    j0 = col0 // cw
    part = pl.BlockSpec((blk, cw), lambda j: (0, j))
    wide = pl.BlockSpec((None, blk, cw), lambda j: (batch_id, 0, j0 + j))
    args, in_specs, aliases = [hidden, own, below, above], [wide, part, part, part], {}
    if result is not None:
        args.append(result)
        in_specs.append(pl.BlockSpec(memory_space=pl.ANY))
        aliases = {4: 0}
    return pl.pallas_call(
        finish_kernel,
        grid=(cols // cw,),
        in_specs=in_specs,
        out_specs=wide,
        out_shape=jax.ShapeDtypeStruct(hidden.shape, BF16),
        input_output_aliases=aliases,
        compiler_params=pltpu.CompilerParams(vmem_limit_bytes=VMEM_LIMIT),
        cost_estimate=pl.CostEstimate(flops=16 * blk * cols, bytes_accessed=12 * blk * cols, transcendentals=0),
        name="finish",
    )(*args)


def solution(mesh):
    tp = mesh.shape["tp"]
    chips = tp // 2
    assert tp == 2 * chips and chips == 4
    pair = [(i, i ^ 1) for i in range(tp)]
    up_ring = [(i, (i + 2) % tp) for i in range(tp)]
    down_ring = [(i, (i - 2) % tp) for i in range(tp)]

    def layer(hidden_blk, attn_gain, attn_bias, mlp_gain, mlp_bias, w_qkv_part, w_out_part, w_up_part, w_down_part, positions):
        batch, seq_rows, width = hidden_blk.shape
        seq = seq_rows * tp
        w_qkv = w_qkv_part.reshape(width, w_qkv_part.shape[2])
        q_cols = w_out_part.shape[0]
        head_dim = (w_qkv.shape[1] - q_cols) // 2
        norms = [v.reshape(1, width) for v in (attn_gain, attn_bias, mlp_gain, mlp_bias)]
        tabs = [t.reshape(tp, seq_rows, LANES) for t in rotary_tables(positions, head_dim)]

        parts = []
        for b in range(batch):
            cut = [(0, seq_rows // 2), (seq_rows // 2, seq_rows)] if b == 0 else [(0, seq_rows)]
            parts += [(b, lo, hi) for lo, hi in cut]
        gathered = [lax.all_gather(hidden_blk[b, lo:hi], "tp", axis=0, tiled=False) for b, lo, hi in parts]

        last_done, result = [positions], [None]

        def in_turn(first):
            out = lax.optimization_barrier((first, last_done[0]))
            if last_done[0] is result:
                result[0] = out[1][0]
            return out[0]

        x32 = hidden_blk.astype(F32)
        mean = jnp.mean(x32, axis=-1, keepdims=True)
        centered = x32 - mean
        rstd = lax.rsqrt(jnp.mean(centered * centered, axis=-1, keepdims=True) + 1e-5)
        stats = lax.all_gather(jnp.stack([mean[..., 0], rstd[..., 0]]), "tp", axis=2, tiled=False)
        stats = jnp.broadcast_to(stats[..., None], (2, batch, tp, seq_rows, LANES))

        expanded = [None] * batch

        def run_expand(b):
            for (pb, lo, hi), xg in zip(parts, gathered):
                if pb == b:
                    expanded[b] = expand(in_turn(xg), b, lo, seq_rows, stats, norms, w_qkv, w_up_part, tabs, expanded[b])
                    last_done[0] = expanded[b][1]

        me = lax.axis_index("tp")
        chip, core = me // 2, me % 2
        targets = jnp.stack([(chip + 2) % chips, (chip + 1) % chips, (chip + chips - 1) % chips, chip]).astype(jnp.int32)
        own_order = targets * 2 + core
        pair_order = targets * 2 + (1 - core)
        ring_up = lambda v: lax.ppermute(v, "tp", up_ring)
        ring_down = lambda v: lax.ppermute(v, "tp", down_ring)

        ctxs, arrived, started, merged = {}, {}, {}, {}

        def run_attend(b):
            q, kv, _ = expanded[b]
            q = in_turn(q)
            ctx = attend(q.reshape(seq, q_cols), kv.reshape(seq, LANES), head_dim)
            last_done[0] = ctx
            ctxs[b] = ctx.reshape(tp, seq_rows, q_cols)

        def run_pair(span):
            b, c, w = span
            (send,) = contract(in_turn(pair_order), ctxs[b], expanded[b][2], w_out_part, w_down_part, c, w)
            last_done[0] = send
            arrived[span] = lax.ppermute(send, "tp", pair)

        def run_own(span):
            b, c, w = span
            pb, pc, pw = next(p for p in arrived if p[0] == b and p[1] <= c and c + w <= p[1] + p[2])
            far_lo, far_hi, up, down, up_lo, down_hi, own = contract(
                in_turn(own_order), ctxs[b], expanded[b][2], w_out_part, w_down_part, c, w, arrived[pb, pc, pw], c - pc)
            last_done[0] = far_lo
            started[span] = (up_lo, down_hi, ring_up(far_lo), ring_down(far_hi), up, down, own)

        def run_merge(span):
            up_lo, down_hi, below, above, up, down, own = started[span]
            up, down = merge(in_turn(up_lo), down_hi, below, above, up, down)
            last_done[0] = up
            merged[span] = (own, ring_up(up), ring_down(down))

        def run_finish(span):
            own, below, above = merged[span]
            result[0] = finish(hidden_blk, span[0], span[1], in_turn(own), below, above, result[0])
            last_done[0] = result

        whole = [(b, 0, width) for b in range(batch)]
        last, half, quarter = batch - 1, width // 2, width // 4
        pairs = [(last, 0, half), (last, half, half)]
        ends = [(last, 0, half), (last, half, quarter), (last, half + quarter, quarter)]
        run_expand(0)
        run_attend(0)
        run_pair(whole[0])
        for b in range(1, batch):
            run_expand(b)
            if b >= 2:
                run_finish(whole[b - 2])
            run_own(whole[b - 1])
            run_attend(b)
            if b < last:
                run_pair(whole[b])
            run_merge(whole[b - 1])
        run_pair(pairs[0])
        run_pair(pairs[1])
        run_own(ends[0])
        run_finish(whole[last - 1])
        run_own(ends[1])
        run_merge(ends[0])
        run_own(ends[2])
        run_merge(ends[1])
        run_finish(ends[0])
        run_merge(ends[2])
        run_finish(ends[1])
        run_finish(ends[2])
        return result[0]

    return jax.shard_map(
        layer, mesh=mesh,
        in_specs=(P("dp", "tp", None), P(), P(), P(), P(), P(None, "tp", None), P("tp", None), P(None, "tp"), P("tp", None), P()),
        out_specs=P("dp", "tp", None), check_vma=False)
```
